32 devices in a mesh: rep: 4 (over y, x), tile: 8 (over z, core).
Axes of the slice: x: 2, y: 2, z: 4, core: 2. Of those that a mesh axis runs over, the one named last changes fastest.
Arguments:
- spins_in: float32 [4, 2048, 4096], P('rep', 'tile'), may hold values from -1 to 1
- noise: bfloat16 [2, 4, 2048, 4096], P(None, 'rep', 'tile'), may hold values from -1.5 to 1.5
- betas: float32 [4], replicated, as said below
- labels: int32 [4], P('rep'), may hold values from 0 to 3, each once
- accept: int32 [2, 4], P(None, 'rep'), may hold values 0 or 1
Outputs:
- spins: float32 [4, 2048, 4096], P('rep', 'tile')
- energy_rows: float32 [4, 2048], P('rep', 'tile')
- margin_rows: float32 [4, 2048], P('rep', 'tile')
- new_labels: int32 [4], P('rep')
- log_ratio: float32 [4], P('rep')
- new_beta: float32 [4], P('rep')
The draws below stay inside these ranges and needn't reach their ends.
Inputs may be any that keep to these rules, and one draw needn't show every extreme that they name: `labels`: a permutation of the temperature indices. `accept`: entry [p, r] is read only where r mod 2 equals p. `betas`: distinct and positive.
All inputs are finite; a program needn't handle non-finite values. No bound on the sum of `accept` on one device may be relied on, other than what follows from the above.
Results may differ from the reference program's by a relative error of at most 0.0003.
Values sent between devices are 32-bit elements; how exact they have to be, the bound alone decides.
A program may use at most 64 MiB of HBM per device.

```python
import jax
import jax.numpy as jnp
from jax import lax

COLS = 4096
SWEEPS = 2
ROWS = 2048
REPLICAS = 4


def draw_betas(key, part):
    steps = jnp.arange(REPLICAS, dtype=jnp.float32) / (REPLICAS - 1)
    ladder_values = 0.2 * jnp.exp(steps * jnp.log(5.0))
    jitter = jax.random.uniform(jax.random.fold_in(key, 11), (REPLICAS,), jnp.float32, 0.99, 1.01)
    return (ladder_values * jitter).astype(jnp.float32)


def touch_ends(array, rng, least, high):
    index_at = [jax.random.randint(jax.random.fold_in(rng, axis), (), 0, length) for axis, length in enumerate(array.shape)]
    longest = array.shape.index(max(array.shape))
    next_to = index_at[:longest] + [(index_at[longest] + 1) % array.shape[longest]] + index_at[longest + 1:]
    return array.at[tuple(index_at)].set(least).at[tuple(next_to)].set(high)


def steps_of(rng, extent, pieces, least, largest):
    factor_of = 1.0
    for dim, parts in pieces:
        heights = jax.random.uniform(jax.random.fold_in(jax.random.fold_in(rng, 6), dim), (parts,), jnp.float32, least / len(pieces), largest / len(pieces))
        factor_of = factor_of * jnp.repeat(jnp.exp(heights), extent[dim] // parts).reshape((-1,) + (1,) * (len(extent) - 1 - dim))
    return factor_of


def setup_inputs(seed: int = 0) -> dict:
    arg_keys = jax.random.split(jax.random.key(seed), 6)
    return {
        "spins_in": jnp.clip(jax.random.uniform(arg_keys[0], (REPLICAS, ROWS, COLS), jnp.float32, -1.0, 1.0) * steps_of(arg_keys[0], (REPLICAS, ROWS, COLS), ((0, 4), (1, 8)), -0.4, 0.0), -1.0, 1.0),
        "noise": jnp.clip(jax.random.uniform(arg_keys[1], (SWEEPS, REPLICAS, ROWS, COLS), jnp.float32, -1.5, 1.5) * steps_of(arg_keys[1], (SWEEPS, REPLICAS, ROWS, COLS), ((1, 4), (2, 8)), -0.4, 0.0), -1.5, 1.5).astype(jnp.bfloat16),
        "betas": draw_betas(jax.random.fold_in(arg_keys[5], 71), 0),
        "labels": jax.random.permutation(arg_keys[3], REPLICAS).astype(jnp.int32),
        "accept": touch_ends((jax.random.randint(arg_keys[4], (2, REPLICAS), 0, 2) < 1).astype(jnp.int32), jax.random.fold_in(arg_keys[4], 1), 0, 1),
    }


def ladder(energy, labels, accept, betas):
    count = energy.shape[0]
    slots = jnp.arange(count, dtype=jnp.int32)
    even = slots % 2 == 0
    accept_zero = accept[0]
    accept_one = accept[1]

    def beta_of(label_set):
        return jnp.sum(jnp.where(label_set[:, None] == slots[None, :], betas[None, :], 0.0), axis=1)

    e_next = jnp.roll(energy, -1)
    beta_zero = beta_of(labels)
    log_zero = (beta_zero - jnp.roll(beta_zero, -1)) * (energy - e_next)
    swap_zero = jnp.where(even, accept_zero, jnp.roll(accept_zero, 1))
    labels_one = jnp.where(swap_zero == 1, jnp.where(even, jnp.roll(labels, -1), jnp.roll(labels, 1)), labels)
    beta_one = beta_of(labels_one)
    log_one = (beta_one - jnp.roll(beta_one, -1)) * (energy - e_next)
    swap_one = jnp.where(even, jnp.roll(accept_one, 1), accept_one)
    labels_two = jnp.where(swap_one == 1, jnp.where(even, jnp.roll(labels_one, 1), jnp.roll(labels_one, -1)), labels_one)
    return labels_two.astype(jnp.int32), jnp.where(even, log_zero, log_one), beta_of(labels_two)


def sweep_one(lattice, noise_rep, beta):
    rows, cols = lattice.shape
    parity = (lax.broadcasted_iota(jnp.int32, (rows, cols), 0) + lax.broadcasted_iota(jnp.int32, (rows, cols), 1)) % 2
    for sweep in range(SWEEPS):
        for colour in range(2):
            field = jnp.roll(lattice, 1, 0) + jnp.roll(lattice, -1, 0) + jnp.roll(lattice, 1, 1) + jnp.roll(lattice, -1, 1)
            fresh = jnp.tanh(beta * field + noise_rep[sweep].astype(jnp.float32))
            lattice = jnp.where(parity == colour, fresh, lattice)
    bonds = jnp.roll(lattice, -1, 0) + jnp.roll(lattice, -1, 1)
    return lattice, -jnp.mean(lattice * bonds, axis=1)


def reference(spins_in, noise, betas, labels, accept):
    count = spins_in.shape[0]
    slots = jnp.arange(count, dtype=jnp.int32)

    def one_replica(index):
        beta = jnp.sum(jnp.where(slots == labels[index], betas, 0.0))
        return sweep_one(spins_in[index], noise[:, index], beta)

    spins, energy_rows = lax.map(one_replica, slots)

    def one_pair(index):
        partner = (index + 1) % count
        return jnp.mean(spins[index] * spins[partner], axis=1)

    margin_rows = lax.map(one_pair, slots)
    energy = jnp.mean(energy_rows, axis=1)
    new_labels, log_ratio, new_beta = ladder(energy, labels, accept, betas)
    return spins, energy_rows, margin_rows, new_labels, log_ratio, new_beta
```

```python
import functools

import jax
import jax.numpy as jnp
from jax import lax
from jax.experimental import pallas as pl
from jax.experimental.pallas import tpu as pltpu
from jax.sharding import PartitionSpec as P

SWEEPS = 2
H = 16
LANES = 128
STAGES = 2 * SWEEPS
MESH = pl.DeviceIdType.MESH


def fold_lanes(value):
    total = value[:, :LANES]
    for k in range(1, value.shape[1] // LANES):
        total = total + value[:, k * LANES : (k + 1) * LANES]
    return total


def with_sides(ref, t, start, width, cols):
    before = (start - LANES) % cols
    after = (start + width) % cols
    return jnp.concatenate(
        [
            ref[t, :, before : before + LANES],
            ref[t, :, start : start + width],
            ref[t, :, after : after + LANES],
        ],
        axis=1,
    )


def kernel(
    n, peers, total_rows,
    spins_ref, noise_ref, betas_ref, labels_ref, accept_ref,
    out_ref, energy_ref, margin_ref, label_out, log_out, beta_out,
    S, N, R, NH, NR, EP, MP, MR, EM, EG, LM, LG,
    s_sem, n_sem, o_sem, hs_sem, hr_sem, bs_sem, br_sem,
    ms_sem, mr_sem, es_sem, er_sem, ls_sem, lr_sem,
):
    _, rows, cols = spins_ref.shape
    T = rows // H
    width = min(1024, cols)
    me = lax.axis_index("rep")
    tile = lax.axis_index("tile")
    nxt = lax.rem(tile + 1, peers)
    prv = lax.rem(tile + peers - 1, peers)

    def load_spins(t):
        return pltpu.make_async_copy(spins_ref.at[0, pl.ds(pl.multiple_of(t * H, H), H)], S.at[t + 1], s_sem.at[t])

    def load_noise(w, t):
        return pltpu.make_async_copy(
            noise_ref.at[w, 0, pl.ds(pl.multiple_of(t * H, H), H)], N.at[w, t + 1], n_sem.at[w, t]
        )

    def load(t):
        load_spins(t).start()
        for w in range(SWEEPS):
            load_noise(w, t).start()

    def loaded(t):
        load_spins(t).wait()
        for w in range(SWEEPS):
            load_noise(w, t).wait()

    barrier = pltpu.get_barrier_semaphore()

    @pl.loop(1, peers)
    def _(d):
        pl.semaphore_signal(barrier, inc=1, device_id={"tile": lax.rem(tile + d, peers)}, device_id_type=MESH)

    @pl.loop(1, n)
    def _(d):
        pl.semaphore_signal(barrier, inc=1, device_id={"rep": lax.rem(me + d, n)}, device_id_type=MESH)

    load(0)
    load(T - 1)

    @pl.loop(1, T - 1)
    def _(t):
        load(t)

    beta = jnp.float32(0.0)
    for k in range(n):
        beta = beta + jnp.where(labels_ref[0] == k, betas_ref[k], 0.0)

    loaded(0)
    loaded(T - 1)
    for w in range(SWEEPS):
        NH[0, w] = N[w, T].astype(jnp.float32)
        NH[1, w] = N[w, 1].astype(jnp.float32)

    pl.semaphore_wait(barrier, n - 1 + peers - 1)

    def halo_copies():
        copies = []
        for side, (start, slot, dev) in enumerate(((rows - H, 0, nxt), (0, T + 1, prv))):
            copies.append(
                pltpu.make_async_remote_copy(
                    spins_ref.at[0, pl.ds(start, H)], S.at[slot], hs_sem.at[side, 0], hr_sem.at[side, 0],
                    device_id={"tile": dev}, device_id_type=MESH,
                )
            )
            for w in range(SWEEPS):
                copies.append(
                    pltpu.make_async_remote_copy(
                        NH.at[side, w], NR.at[side, w], hs_sem.at[side, 1 + w], hr_sem.at[side, 1 + w],
                        device_id={"tile": dev}, device_id_type=MESH,
                    )
                )
        return copies

    halos = halo_copies()
    for copy in halos:
        copy.start()

    def bulk(t):
        dest = lax.rem(t, n)
        q = t // n
        return pltpu.make_async_remote_copy(
            S.at[t + 1], R.at[me, q], bs_sem.at[t], br_sem.at[me, q],
            device_id={"rep": dest}, device_id_type=MESH,
        )

    def store_out(t):
        return pltpu.make_async_copy(S.at[t + 1], out_ref.at[0, pl.ds(pl.multiple_of(t * H, H), H)], o_sem.at[t])

    row = lax.broadcasted_iota(jnp.int32, (H, width), 0)
    parity = (row + lax.broadcasted_iota(jnp.int32, (H, width), 1)) % 2

    def update(t, stage):
        sweep, colour = stage // 2, stage % 2
        i = t + 1
        above = jnp.maximum(i - 1, 0)
        below = jnp.minimum(i + 1, T + 1)
        for b in range(cols // width):
            c0 = b * width
            cs = slice(c0, c0 + width)
            ext = with_sides(S, i, c0, width, cols)
            cur = ext[:, LANES : LANES + width]
            left = pltpu.roll(ext, 1, 1)[:, LANES : LANES + width]
            right = pltpu.roll(ext, width + 2 * LANES - 1, 1)[:, LANES : LANES + width]
            up = jnp.where(row == 0, S[above, H - 1 : H, cs], pltpu.roll(cur, 1, 0))
            down = jnp.where(row == H - 1, S[below, 0:1, cs], pltpu.roll(cur, H - 1, 0))
            field = (up + down) + (left + right)
            fresh = jnp.tanh(beta * field + N[sweep, i, :, cs].astype(jnp.float32))
            S[i, :, cs] = jnp.where(parity == colour, fresh, cur)

    def finish(t):
        i = t + 1

        @pl.when(lax.rem(t, n) != me)
        def _():
            bulk(t).start()

        store_out(t).start()
        total = jnp.zeros((H, LANES), jnp.float32)
        for b in range(cols // width):
            c0 = b * width
            cs = slice(c0, c0 + width)
            cur = S[i, :, cs]
            after = (c0 + width) % cols
            ext = jnp.concatenate([cur, S[i, :, after : after + LANES]], axis=1)
            right = pltpu.roll(ext, width + LANES - 1, 1)[:, :width]
            down = jnp.where(row == H - 1, S[i + 1, 0:1, cs], pltpu.roll(cur, H - 1, 0))
            total = total + fold_lanes(cur * (down + right))
        EP[t] = total

    loaded(1)

    @pl.loop(1, T + STAGES)
    def _(s):
        @pl.when(s + 1 < T - 1)
        def _():
            loaded(s + 1)

        @pl.when(s == T - 1)
        def _():
            for copy in halos[1 + SWEEPS :]:
                copy.wait_recv()
            for w in range(SWEEPS):
                N[w, T + 1] = NR[1, w].astype(jnp.bfloat16)

        for k in range(STAGES):
            t = s - k

            @pl.when((t >= k + 1) & (t <= T))
            def _():
                update(t, k)

        @pl.when(s - STAGES >= STAGES)
        def _():
            finish(s - STAGES)

    for copy in halos[: 1 + SWEEPS]:
        copy.wait_recv()
    for w in range(SWEEPS):
        N[w, 0] = NR[0, w].astype(jnp.bfloat16)

    for k in range(STAGES):

        @pl.loop(-1 if k < STAGES - 1 else 0, k + 1)
        def _(t):
            update(t, k)

    @pl.loop(0, STAGES)
    def _(t):
        finish(t)

    per_row = jnp.sum(EP[...].reshape(rows, LANES).T, axis=0, keepdims=True) * (-1.0 / cols)
    energy_ref[...] = per_row
    local = jnp.broadcast_to(jnp.sum(per_row, axis=1, keepdims=True), (8, LANES))
    EM[...] = local
    EG[tile] = local

    def energy_copy(d):
        return pltpu.make_async_remote_copy(
            EM, EG.at[tile], es_sem.at[d], er_sem.at[tile],
            device_id={"tile": lax.rem(tile + d, peers)}, device_id_type=MESH,
        )

    def energy_from(d):
        src = lax.rem(tile + d, peers)
        return pltpu.make_async_remote_copy(
            EM, EG.at[src], es_sem.at[d], er_sem.at[src], device_id={"tile": src}, device_id_type=MESH
        )

    @pl.loop(1, peers)
    def _(d):
        energy_copy(d).start()

    @pl.loop(1, peers)
    def _(d):
        energy_from(d).wait_recv()

    energy = jnp.sum(EG[...], axis=0) / total_rows
    line = lax.broadcasted_iota(jnp.int32, (8, LANES), 0)
    label_float = labels_ref[0].astype(jnp.float32)
    accept_zero = accept_ref[0, 0].astype(jnp.float32)
    accept_one = accept_ref[1, 0].astype(jnp.float32)
    message = jnp.where(
        line == 0, energy,
        jnp.where(line == 1, label_float, jnp.where(line == 2, accept_zero, accept_one)),
    )
    LM[...] = message
    LG[me] = message

    def ladder_copy(d):
        return pltpu.make_async_remote_copy(
            LM, LG.at[me], ls_sem.at[d], lr_sem.at[me],
            device_id={"rep": lax.rem(me + d, n)}, device_id_type=MESH,
        )

    def ladder_from(d):
        src = lax.rem(me + d, n)
        return pltpu.make_async_remote_copy(
            LM, LG.at[src], ls_sem.at[d], lr_sem.at[src], device_id={"rep": src}, device_id_type=MESH
        )

    @pl.loop(1, n)
    def _(d):
        ladder_copy(d).start()

    def margin_copy(q, d):
        dest = lax.rem(me + d, n)
        return pltpu.make_async_remote_copy(
            MP.at[dest, q], MR.at[q * n + me], ms_sem.at[q, d], mr_sem.at[q * n + me],
            device_id={"rep": dest}, device_id_type=MESH,
        )

    def margin_from(t):
        src = lax.rem(t, n)
        return pltpu.make_async_remote_copy(
            MP.at[0, 0], MR.at[t], ms_sem.at[0, 1], mr_sem.at[t], device_id={"rep": src}, device_id_type=MESH
        )

    def bulk_from(src, q):
        return pltpu.make_async_remote_copy(
            S.at[1], R.at[src, q], bs_sem.at[0], br_sem.at[src, q], device_id={"rep": src}, device_id_type=MESH
        )

    @pl.loop(0, T // n)
    def _(q):
        R[me, q] = S[q * n + me + 1]

        @pl.loop(1, n)
        def _(d):
            bulk_from(lax.rem(me + d, n), q).wait_recv()

        totals = [jnp.zeros((H, LANES), jnp.float32) for _ in range(n)]
        chunk = min(512, cols)
        for b in range(cols // chunk):
            cs = slice(b * chunk, (b + 1) * chunk)
            parts = [R[r, q, :, cs] for r in range(n)]
            for r in range(n):
                totals[r] = totals[r] + fold_lanes(parts[r] * parts[(r + 1) % n])
        for r in range(n):
            MP[r, q] = totals[r]
        MR[q * n + me] = MP[me, q]

        @pl.loop(1, n)
        def _(d):
            margin_copy(q, d).start()

    @pl.loop(1, n)
    def _(d):
        ladder_from(d).wait_recv()

    energies = [LG[r][0:1] for r in range(n)]
    labels = [LG[r][1:2] for r in range(n)]
    acc = [[LG[r][2 + p : 3 + p] for r in range(n)] for p in range(2)]

    def beta_of(label):
        value = jnp.zeros((1, LANES), jnp.float32)
        for k in range(n):
            value = value + jnp.where(label == float(k), betas_ref[k], 0.0)
        return value

    def swapped(current, accepts, first):
        result = list(current)
        for r in range(first, n, 2):
            o = (r + 1) % n
            take = accepts[r] == 1.0
            result[r] = jnp.where(take, current[o], current[r])
            result[o] = jnp.where(take, current[r], current[o])
        return result

    labels_one = swapped(labels, acc[0], 0)
    labels_two = swapped(labels_one, acc[1], 1)
    zero = [beta_of(x) for x in labels]
    one = [beta_of(x) for x in labels_one]
    two = [beta_of(x) for x in labels_two]
    my_label = jnp.zeros((1, LANES), jnp.float32)
    my_log = my_label
    my_beta = my_label
    for r in range(n):
        o = (r + 1) % n
        betas_here = zero if r % 2 == 0 else one
        log = (betas_here[r] - betas_here[o]) * (energies[r] - energies[o])
        my_label = jnp.where(me == r, labels_two[r], my_label)
        my_log = jnp.where(me == r, log, my_log)
        my_beta = jnp.where(me == r, two[r], my_beta)
    label_out[0] = jnp.max(my_label).astype(jnp.int32)
    log_out[0] = jnp.max(my_log)
    beta_out[0] = jnp.max(my_beta)

    for copy in halos:
        copy.wait_send()

    @pl.loop(0, T)
    def _(t):
        store_out(t).wait()

        @pl.when(lax.rem(t, n) != me)
        def _():
            bulk(t).wait_send()

    @pl.loop(1, peers)
    def _(d):
        energy_copy(d).wait_send()

    @pl.loop(1, n)
    def _(d):
        ladder_copy(d).wait_send()

    @pl.loop(0, T)
    def _(t):
        @pl.when(lax.rem(t, n) != me)
        def _():
            margin_from(t).wait_recv()

    @pl.loop(0, T // n)
    def _(q):
        @pl.loop(1, n)
        def _(d):
            margin_copy(q, d).wait_send()

    margin_ref[...] = jnp.sum(MR[...].reshape(rows, LANES).T, axis=0, keepdims=True) * (1.0 / cols)


def body(n, peers, total_rows, spins_in, noise, betas, labels, accept):
    _, rows, cols = spins_in.shape
    T = rows // H
    f32 = jnp.float32
    hbm = pl.BlockSpec(memory_space=pltpu.HBM)
    smem = pl.BlockSpec(memory_space=pltpu.SMEM)
    vmem = pl.BlockSpec(memory_space=pltpu.VMEM)
    dma = pltpu.SemaphoreType.DMA
    outs = pl.pallas_call(
        functools.partial(kernel, n, peers, total_rows),
        out_shape=(
            jax.ShapeDtypeStruct(spins_in.shape, f32),
            jax.ShapeDtypeStruct((1, rows), f32),
            jax.ShapeDtypeStruct((1, rows), f32),
            jax.ShapeDtypeStruct((1,), jnp.int32),
            jax.ShapeDtypeStruct((1,), f32),
            jax.ShapeDtypeStruct((1,), f32),
        ),
        in_specs=[hbm, hbm, smem, smem, smem],
        out_specs=(hbm, vmem, vmem, smem, smem, smem),
        scratch_shapes=[
            pltpu.VMEM((T + 2, H, cols), f32),
            pltpu.VMEM((SWEEPS, T + 2, H, cols), jnp.bfloat16),
            pltpu.VMEM((n, T // n, H, cols), f32),
            pltpu.VMEM((2, SWEEPS, H, cols), f32),
            pltpu.VMEM((2, SWEEPS, H, cols), f32),
            pltpu.VMEM((T, H, LANES), f32),
            pltpu.VMEM((n, T // n, H, LANES), f32),
            pltpu.VMEM((T, H, LANES), f32),
            pltpu.VMEM((8, LANES), f32),
            pltpu.VMEM((peers, 8, LANES), f32),
            pltpu.VMEM((8, LANES), f32),
            pltpu.VMEM((n, 8, LANES), f32),
            dma((T,)),
            dma((SWEEPS, T)),
            dma((T,)),
            dma((2, 1 + SWEEPS)),
            dma((2, 1 + SWEEPS)),
            dma((T,)),
            dma((n, T // n)),
            dma((T // n, n)),
            dma((T,)),
            dma((peers,)),
            dma((peers,)),
            dma((n,)),
            dma((n,)),
        ],
        compiler_params=pltpu.CompilerParams(collective_id=0, has_side_effects=True),
        name="lattice_exchange",
    )(spins_in, noise, betas, labels, accept)
    return outs


def solution(mesh):
    n = mesh.shape["rep"]
    peers = mesh.shape["tile"]
    in_specs = (P("rep", "tile", None), P(None, "rep", "tile", None), P(), P("rep"), P(None, "rep"))
    out_specs = (P("rep", "tile", None), P("rep", "tile"), P("rep", "tile"), P("rep"), P("rep"), P("rep"))

    def run(spins_in, noise, betas, labels, accept):
        total_rows = spins_in.shape[1]
        step = jax.shard_map(
            functools.partial(body, n, peers, total_rows),
            mesh=mesh, in_specs=in_specs, out_specs=out_specs, check_vma=False,
        )
        return step(spins_in, noise, betas, labels, accept)

    return run
```

```python
import functools

import jax
import jax.numpy as jnp
from jax import lax
from jax.experimental import pallas as pl
from jax.experimental.pallas import tpu as pltpu
from jax.sharding import PartitionSpec as P

SWEEPS = 2
H = 16
HALO = 8
LANES = 128
STAGES = 2 * SWEEPS
MESH = pl.DeviceIdType.MESH


def fold_lanes(value):
    total = value[:, :LANES]
    for k in range(1, value.shape[1] // LANES):
        total = total + value[:, k * LANES : (k + 1) * LANES]
    return total


def with_sides(ref, t, start, width, cols):
    before = (start - LANES) % cols
    after = (start + width) % cols
    return jnp.concatenate(
        [
            ref[t, :, before : before + LANES],
            ref[t, :, start : start + width],
            ref[t, :, after : after + LANES],
        ],
        axis=1,
    )


def kernel(
    n, peers, total_rows,
    spins_ref, noise_ref, betas_hbm, labels_ref, accept_hbm,
    out_ref, energy_ref, margin_ref, label_out, log_out, beta_out,
    S, N, R, NH, NR, EP, MP, MS, MR, EM, EG, LM, LG, betas_ref, accept_ref,
    s_sem, n_sem, o_sem, hs_sem, hr_sem, bs_sem, br_sem,
    ms_sem, mr_sem, es_sem, er_sem, ls_sem, lr_sem, i_sem,
):
    _, rows, cols = spins_ref.shape
    T = rows // H
    width = min(1024, cols)
    share = cols // n
    me = lax.axis_index("rep")
    tile = lax.axis_index("tile")
    nxt = lax.rem(tile + 1, peers)
    prv = lax.rem(tile + peers - 1, peers)

    def load_spins(t):
        return pltpu.make_async_copy(spins_ref.at[0, pl.ds(pl.multiple_of(t * H, H), H)], S.at[t + 1], s_sem.at[t])

    def load_noise(w, t):
        return pltpu.make_async_copy(
            noise_ref.at[w, 0, pl.ds(pl.multiple_of(t * H, H), H)], N.at[w, t + 1], n_sem.at[w, t]
        )

    def load(t):
        load_spins(t).start()
        for w in range(SWEEPS):
            load_noise(w, t).start()

    def loaded(t):
        load_spins(t).wait()
        for w in range(SWEEPS):
            load_noise(w, t).wait()

    barrier = pltpu.get_barrier_semaphore()

    @pl.loop(1, peers)
    def _(d):
        pl.semaphore_signal(barrier, inc=1, device_id={"tile": lax.rem(tile + d, peers)}, device_id_type=MESH)

    @pl.loop(1, n)
    def _(d):
        pl.semaphore_signal(barrier, inc=1, device_id={"rep": lax.rem(me + d, n)}, device_id_type=MESH)

    small = [
        pltpu.make_async_copy(src, dst, i_sem.at[k])
        for k, (src, dst) in enumerate(
            ((betas_hbm, betas_ref), (accept_hbm, accept_ref))
        )
    ]
    for copy in small:
        copy.start()
    load(0)
    load(T - 1)

    @pl.loop(1, T - 1)
    def _(t):
        load(t)

    for copy in small:
        copy.wait()
    beta = jnp.float32(0.0)
    for k in range(n):
        beta = beta + jnp.where(labels_ref[0] == k, betas_ref[k], 0.0)

    loaded(0)
    loaded(T - 1)
    for w in range(SWEEPS):
        NH[0, w] = N[w, T].astype(jnp.float32)[H - HALO :]
        NH[1, w] = N[w, 1].astype(jnp.float32)[:HALO]

    pl.semaphore_wait(barrier, n - 1 + peers - 1)

    def halo_copies():
        copies = []
        for side, (start, slot, dev) in enumerate(((rows - HALO, 0, nxt), (0, T + 1, prv))):
            copies.append(
                pltpu.make_async_remote_copy(
                    spins_ref.at[0, pl.ds(start, HALO)], S.at[slot, pl.ds((H - HALO) * (1 - side), HALO)], hs_sem.at[side, 0], hr_sem.at[side, 0],
                    device_id={"tile": dev}, device_id_type=MESH,
                )
            )
            for w in range(SWEEPS):
                copies.append(
                    pltpu.make_async_remote_copy(
                        NH.at[side, w], NR.at[side, w], hs_sem.at[side, 1 + w], hr_sem.at[side, 1 + w],
                        device_id={"tile": dev}, device_id_type=MESH,
                    )
                )
        return copies

    halos = halo_copies()
    for copy in halos:
        copy.start()

    def share_of(d):
        return pl.ds(pl.multiple_of(d * share, LANES), share)

    def bulk(t, d):
        dest = lax.rem(me + d, n)
        return pltpu.make_async_remote_copy(
            S.at[t + 1, :, share_of(dest)], R.at[me, t], bs_sem.at[t, d], br_sem.at[me, t],
            device_id={"rep": dest}, device_id_type=MESH,
        )

    def store_out(t):
        return pltpu.make_async_copy(S.at[t + 1], out_ref.at[0, pl.ds(pl.multiple_of(t * H, H), H)], o_sem.at[t])

    row = lax.broadcasted_iota(jnp.int32, (H, width), 0)
    parity = (row + lax.broadcasted_iota(jnp.int32, (H, width), 1)) % 2

    def update(t, stage):
        sweep, colour = stage // 2, stage % 2
        i = t + 1
        above = jnp.maximum(i - 1, 0)
        below = jnp.minimum(i + 1, T + 1)
        for b in range(cols // width):
            c0 = b * width
            cs = slice(c0, c0 + width)
            ext = with_sides(S, i, c0, width, cols)
            cur = ext[:, LANES : LANES + width]
            left = pltpu.roll(ext, 1, 1)[:, LANES : LANES + width]
            right = pltpu.roll(ext, width + 2 * LANES - 1, 1)[:, LANES : LANES + width]
            up = jnp.where(row == 0, S[above, H - 1 : H, cs], pltpu.roll(cur, 1, 0))
            down = jnp.where(row == H - 1, S[below, 0:1, cs], pltpu.roll(cur, H - 1, 0))
            field = (up + down) + (left + right)
            fresh = jnp.tanh(beta * field + N[sweep, i, :, cs].astype(jnp.float32))
            S[i, :, cs] = jnp.where(parity == colour, fresh, cur)

    def finish(t):
        i = t + 1

        for d in range(1, n):
            bulk(t, d).start()
        store_out(t).start()
        R[me, t] = S[i, :, share_of(me)]
        total = jnp.zeros((H, LANES), jnp.float32)
        for b in range(cols // width):
            c0 = b * width
            cs = slice(c0, c0 + width)
            cur = S[i, :, cs]
            after = (c0 + width) % cols
            ext = jnp.concatenate([cur, S[i, :, after : after + LANES]], axis=1)
            right = pltpu.roll(ext, width + LANES - 1, 1)[:, :width]
            down = jnp.where(row == H - 1, S[i + 1, 0:1, cs], pltpu.roll(cur, H - 1, 0))
            total = total + fold_lanes(cur * (down + right))
        EP[t] = total

    loaded(1)

    @pl.loop(1, T + STAGES)
    def _(s):
        @pl.when(s + 1 < T - 1)
        def _():
            loaded(s + 1)

        @pl.when(s == T - 1)
        def _():
            for copy in halos[1 + SWEEPS :]:
                copy.wait_recv()
            for w in range(SWEEPS):
                N[w, T + 1] = jnp.concatenate([NR[1, w], NR[1, w]], axis=0).astype(jnp.bfloat16)

        for k in range(STAGES):
            t = s - k

            @pl.when((t >= k + 1) & (t <= T))
            def _():
                update(t, k)

        @pl.when(s - STAGES >= STAGES)
        def _():
            finish(s - STAGES)

    for copy in halos[: 1 + SWEEPS]:
        copy.wait_recv()
    for w in range(SWEEPS):
        N[w, 0] = jnp.concatenate([NR[0, w], NR[0, w]], axis=0).astype(jnp.bfloat16)

    for k in range(STAGES):

        @pl.loop(-1 if k < STAGES - 1 else 0, k + 1)
        def _(t):
            update(t, k)

    @pl.loop(0, STAGES)
    def _(t):
        finish(t)

    per_row = jnp.sum(EP[...].reshape(rows, LANES).T, axis=0, keepdims=True) * (-1.0 / cols)
    energy_ref[...] = per_row
    local = jnp.broadcast_to(jnp.sum(per_row, axis=1, keepdims=True), (8, LANES))
    EM[...] = local
    EG[tile] = local

    def energy_copy(d):
        return pltpu.make_async_remote_copy(
            EM, EG.at[tile], es_sem.at[d], er_sem.at[tile],
            device_id={"tile": lax.rem(tile + d, peers)}, device_id_type=MESH,
        )

    def energy_from(d):
        src = lax.rem(tile + d, peers)
        return pltpu.make_async_remote_copy(
            EM, EG.at[src], es_sem.at[d], er_sem.at[src], device_id={"tile": src}, device_id_type=MESH
        )

    @pl.loop(1, peers)
    def _(d):
        energy_copy(d).start()

    @pl.loop(1, peers)
    def _(d):
        energy_from(d).wait_recv()

    energy = jnp.sum(EG[...], axis=0) / total_rows
    line = lax.broadcasted_iota(jnp.int32, (8, LANES), 0)
    label_float = labels_ref[0].astype(jnp.float32)
    accept_zero = accept_ref[0, 0].astype(jnp.float32)
    accept_one = accept_ref[0, 1].astype(jnp.float32)
    message = jnp.where(
        line == 0, energy,
        jnp.where(line == 1, label_float, jnp.where(line == 2, accept_zero, accept_one)),
    )
    LM[...] = message
    LG[me] = message

    def ladder_copy(d):
        return pltpu.make_async_remote_copy(
            LM, LG.at[me], ls_sem.at[d], lr_sem.at[me],
            device_id={"rep": lax.rem(me + d, n)}, device_id_type=MESH,
        )

    def ladder_from(d):
        src = lax.rem(me + d, n)
        return pltpu.make_async_remote_copy(
            LM, LG.at[src], ls_sem.at[d], lr_sem.at[src], device_id={"rep": src}, device_id_type=MESH
        )

    @pl.loop(1, n)
    def _(d):
        ladder_copy(d).start()

    def bulk_from(d, t):
        src = lax.rem(me + d, n)
        return pltpu.make_async_remote_copy(
            S.at[1, :, share_of(0)], R.at[src, t], bs_sem.at[0, 1], br_sem.at[src, t],
            device_id={"rep": src}, device_id_type=MESH,
        )

    @pl.loop(STAGES, T + STAGES)
    def _(s):
        t = lax.rem(s, T)
        for d in range(1, n):
            bulk_from(d, t).wait_recv()
        totals = [jnp.zeros((H, LANES), jnp.float32) for _ in range(n)]
        for b in range(share // LANES):
            cs = slice(b * LANES, (b + 1) * LANES)
            parts = [R[r, t, :, cs] for r in range(n)]
            for r in range(n):
                totals[r] = totals[r] + parts[r] * parts[(r + 1) % n]
        for r in range(n):
            MP[r, t] = totals[r]

    for r in range(n):
        sums = jnp.sum(MP[r].reshape(rows, LANES).T, axis=0, keepdims=True)
        MS[r] = jnp.broadcast_to(sums, (8, rows))
    MR[me] = MS[me]

    def margin_copy(d):
        dest = lax.rem(me + d, n)
        return pltpu.make_async_remote_copy(
            MS.at[dest], MR.at[me], ms_sem.at[d], mr_sem.at[me], device_id={"rep": dest}, device_id_type=MESH
        )

    def margin_from(d):
        src = lax.rem(me + d, n)
        return pltpu.make_async_remote_copy(
            MS.at[0], MR.at[src], ms_sem.at[d], mr_sem.at[src], device_id={"rep": src}, device_id_type=MESH
        )

    for d in range(1, n):
        margin_copy(d).start()

    @pl.loop(1, n)
    def _(d):
        ladder_from(d).wait_recv()

    energies = [LG[r][0:1] for r in range(n)]
    labels = [LG[r][1:2] for r in range(n)]
    acc = [[LG[r][2 + p : 3 + p] for r in range(n)] for p in range(2)]

    def beta_of(label):
        value = jnp.zeros((1, LANES), jnp.float32)
        for k in range(n):
            value = value + jnp.where(label == float(k), betas_ref[k], 0.0)
        return value

    def swapped(current, accepts, first):
        result = list(current)
        for r in range(first, n, 2):
            o = (r + 1) % n
            take = accepts[r] == 1.0
            result[r] = jnp.where(take, current[o], current[r])
            result[o] = jnp.where(take, current[r], current[o])
        return result

    labels_one = swapped(labels, acc[0], 0)
    labels_two = swapped(labels_one, acc[1], 1)
    zero = [beta_of(x) for x in labels]
    one = [beta_of(x) for x in labels_one]
    two = [beta_of(x) for x in labels_two]
    my_label = jnp.zeros((1, LANES), jnp.float32)
    my_log = my_label
    my_beta = my_label
    for r in range(n):
        o = (r + 1) % n
        betas_here = zero if r % 2 == 0 else one
        log = (betas_here[r] - betas_here[o]) * (energies[r] - energies[o])
        my_label = jnp.where(me == r, labels_two[r], my_label)
        my_log = jnp.where(me == r, log, my_log)
        my_beta = jnp.where(me == r, two[r], my_beta)
    label_out[0] = jnp.max(my_label).astype(jnp.int32)
    log_out[0] = jnp.max(my_log)
    beta_out[0] = jnp.max(my_beta)

    for copy in halos:
        copy.wait_send()

    @pl.loop(0, T)
    def _(t):
        store_out(t).wait()
        for d in range(1, n):
            bulk(t, d).wait_send()

    @pl.loop(1, peers)
    def _(d):
        energy_copy(d).wait_send()

    for d in range(1, n):
        ladder_copy(d).wait_send()
        margin_from(d).wait_recv()
        margin_copy(d).wait_send()

    margin_ref[...] = jnp.sum(MR[...], axis=0)[0:1] * (1.0 / cols)


def settle(spins, *refs):
    count = (len(refs) - 4) // 2
    sources, outs = refs[:count], refs[count + 1 : 2 * count + 1]
    out = refs[count]
    buffer, in_sem, out_sem, small_sem = refs[2 * count + 1 :]
    pieces = buffer.shape[0]
    height = buffer.shape[1]

    def copies(k):
        place = pl.ds(k * height, height)
        return (
            pltpu.make_async_copy(spins.at[0, place], buffer.at[k], in_sem.at[k]),
            pltpu.make_async_copy(buffer.at[k], out.at[0, place], out_sem.at[k]),
        )

    small = [pltpu.make_async_copy(a, b, small_sem.at[k]) for k, (a, b) in enumerate(zip(sources, outs))]
    for k in range(pieces):
        copies(k)[0].start()
    for copy in small:
        copy.start()
    for k in range(pieces):
        copies(k)[0].wait()
        copies(k)[1].start()
    for k in range(pieces):
        copies(k)[1].wait()
    for copy in small:
        copy.wait()


def body(n, peers, total_rows, spins_in, noise, betas, labels, accept):
    _, rows, cols = spins_in.shape
    T = rows // H
    f32 = jnp.float32
    hbm = pl.BlockSpec(memory_space=pltpu.HBM)
    smem = pl.BlockSpec(memory_space=pltpu.SMEM)
    vmem = pl.BlockSpec(memory_space=pltpu.VMEM)
    dma = pltpu.SemaphoreType.DMA
    accept = jnp.transpose(accept)
    results = pl.pallas_call(
        functools.partial(kernel, n, peers, total_rows),
        out_shape=(
            jax.ShapeDtypeStruct(spins_in.shape, f32),
            jax.ShapeDtypeStruct((1, rows), f32),
            jax.ShapeDtypeStruct((1, rows), f32),
            jax.ShapeDtypeStruct((1,), jnp.int32),
            jax.ShapeDtypeStruct((1,), f32),
            jax.ShapeDtypeStruct((1,), f32),
        ),
        in_specs=[hbm, hbm, hbm, smem, hbm],
        out_specs=(hbm, vmem, vmem, smem, smem, smem),
        scratch_shapes=[
            pltpu.VMEM((T + 2, H, cols), f32),
            pltpu.VMEM((SWEEPS, T + 2, H, cols), jnp.bfloat16),
            pltpu.VMEM((n, T, H, cols // n), f32),
            pltpu.VMEM((2, SWEEPS, HALO, cols), f32),
            pltpu.VMEM((2, SWEEPS, HALO, cols), f32),
            pltpu.VMEM((T, H, LANES), f32),
            pltpu.VMEM((n, T, H, LANES), f32),
            pltpu.VMEM((n, 8, rows), f32),
            pltpu.VMEM((n, 8, rows), f32),
            pltpu.VMEM((8, LANES), f32),
            pltpu.VMEM((peers, 8, LANES), f32),
            pltpu.VMEM((8, LANES), f32),
            pltpu.VMEM((n, 8, LANES), f32),
            pltpu.SMEM(betas.shape, f32),
            pltpu.SMEM(accept.shape, jnp.int32),
            dma((T,)),
            dma((SWEEPS, T)),
            dma((T,)),
            dma((2, 1 + SWEEPS)),
            dma((2, 1 + SWEEPS)),
            dma((T, n)),
            dma((n, T)),
            dma((n,)),
            dma((n,)),
            dma((peers,)),
            dma((peers,)),
            dma((n,)),
            dma((n,)),
            dma((2,)),
        ],
        compiler_params=pltpu.CompilerParams(collective_id=0, has_side_effects=True),
        name="lattice_exchange",
    )(spins_in, noise, betas, labels, accept)
    pieces = 8
    return pl.pallas_call(
        settle,
        out_shape=tuple(jax.ShapeDtypeStruct(x.shape, x.dtype) for x in results),
        in_specs=[hbm] * len(results),
        out_specs=(hbm,) * len(results),
        scratch_shapes=[
            pltpu.VMEM((pieces, rows // pieces, cols), f32),
            dma((pieces,)),
            dma((pieces,)),
            dma((len(results) - 1,)),
        ],
        name="settle",
    )(*results)


def solution(mesh):
    n = mesh.shape["rep"]
    peers = mesh.shape["tile"]
    in_specs = (P("rep", "tile", None), P(None, "rep", "tile", None), P(), P("rep"), P(None, "rep"))
    out_specs = (P("rep", "tile", None), P("rep", "tile"), P("rep", "tile"), P("rep"), P("rep"), P("rep"))

    def run(spins_in, noise, betas, labels, accept):
        total_rows = spins_in.shape[1]
        step = jax.shard_map(
            functools.partial(body, n, peers, total_rows),
            mesh=mesh, in_specs=in_specs, out_specs=out_specs, check_vma=False,
        )
        return step(spins_in, noise, betas, labels, accept)

    return run
```

```python
import functools

import jax
import jax.numpy as jnp
from jax import lax
from jax.experimental import pallas as pl
from jax.experimental.pallas import tpu as pltpu
from jax.sharding import PartitionSpec as P

SWEEPS = 2
H = 8
GROUP = 2
LANES = 128
VMEM_BYTES = 60 * 1024 * 1024
STAGES = 2 * SWEEPS
MESH = pl.DeviceIdType.MESH


def fold_lanes(value):
    total = value[:, :LANES]
    for k in range(1, value.shape[1] // LANES):
        total = total + value[:, k * LANES : (k + 1) * LANES]
    return total


def with_sides(ref, t, start, width, cols):
    before = (start - LANES) % cols
    after = (start + width) % cols
    return jnp.concatenate(
        [
            ref[t, :, before : before + LANES],
            ref[t, :, start : start + width],
            ref[t, :, after : after + LANES],
        ],
        axis=1,
    )


def kernel(
    n, peers, total_rows,
    spins_ref, noise_ref, betas_hbm, labels_ref, accept_hbm,
    out_ref, energy_ref, margin_ref, label_out, log_out, beta_out,
    S, N, R, NH, NR, EP, MP, MS, MR, EM, EG, LM, LG, betas_ref, accept_ref,
    s_sem, n_sem, hs_sem, hr_sem, bs_sem, br_sem,
    ms_sem, mr_sem, es_sem, er_sem, ls_sem, lr_sem, i_sem,
):
    _, rows, cols = spins_ref.shape
    T = rows // H
    width = min(1024, cols)
    share = cols // n
    me = lax.axis_index("rep")
    tile = lax.axis_index("tile")
    nxt = lax.rem(tile + 1, peers)
    prv = lax.rem(tile + peers - 1, peers)

    def load_spins(t):
        return pltpu.make_async_copy(spins_ref.at[0, pl.ds(pl.multiple_of(t * H, H), H)], S.at[t + 1], s_sem.at[t])

    def load_noise(w, t):
        return pltpu.make_async_copy(
            noise_ref.at[w, 0, pl.ds(pl.multiple_of(t * H, H), H)], N.at[w, t + 1], n_sem.at[w, t]
        )

    def load(t):
        load_spins(t).start()
        for w in range(SWEEPS):
            load_noise(w, t).start()

    def loaded(t):
        load_spins(t).wait()
        for w in range(SWEEPS):
            load_noise(w, t).wait()

    barrier = pltpu.get_barrier_semaphore()

    @pl.loop(1, peers)
    def _(d):
        pl.semaphore_signal(barrier, inc=1, device_id={"tile": lax.rem(tile + d, peers)}, device_id_type=MESH)

    @pl.loop(1, n)
    def _(d):
        pl.semaphore_signal(barrier, inc=1, device_id={"rep": lax.rem(me + d, n)}, device_id_type=MESH)

    small = [
        pltpu.make_async_copy(src, dst, i_sem.at[k])
        for k, (src, dst) in enumerate(
            ((betas_hbm, betas_ref), (accept_hbm, accept_ref))
        )
    ]
    for copy in small:
        copy.start()
    @pl.loop(0, T)
    def _(t):
        load(t)

    for copy in small:
        copy.wait()
    beta = jnp.float32(0.0)
    for k in range(n):
        beta = beta + jnp.where(labels_ref[0] == k, betas_ref[k], 0.0)

    def halo_copies():
        copies = []
        for side, (start, slot, dev) in enumerate(((rows - H, 0, nxt), (0, T + 1, prv))):
            copies.append(
                pltpu.make_async_remote_copy(
                    spins_ref.at[0, pl.ds(start, H)], S.at[slot], hs_sem.at[side, 0], hr_sem.at[side, 0],
                    device_id={"tile": dev}, device_id_type=MESH,
                )
            )
            for w in range(SWEEPS):
                copies.append(
                    pltpu.make_async_remote_copy(
                        NH.at[side, w], NR.at[side, w], hs_sem.at[side, 1 + w], hr_sem.at[side, 1 + w],
                        device_id={"tile": dev}, device_id_type=MESH,
                    )
                )
        return copies

    halos = halo_copies()

    def share_of(d):
        return pl.ds(pl.multiple_of(d * share, LANES), share)

    def bulk(p, d):
        dest = lax.rem(me + d, n)
        return pltpu.make_async_remote_copy(
            S.at[pl.ds(p * GROUP + 1, GROUP), :, share_of(dest)], R.at[me, pl.ds(p * GROUP, GROUP)],
            bs_sem.at[p, d], br_sem.at[me, p],
            device_id={"rep": dest}, device_id_type=MESH,
        )

    row = lax.broadcasted_iota(jnp.int32, (H, width), 0)
    parity = (row + lax.broadcasted_iota(jnp.int32, (H, width), 1)) % 2

    def update(t, stage):
        sweep, colour = stage // 2, stage % 2
        i = t + 1
        above = jnp.maximum(i - 1, 0)
        below = jnp.minimum(i + 1, T + 1)
        for b in range(cols // width):
            c0 = b * width
            cs = slice(c0, c0 + width)
            ext = with_sides(S, i, c0, width, cols)
            cur = ext[:, LANES : LANES + width]
            left = pltpu.roll(ext, 1, 1)[:, LANES : LANES + width]
            right = pltpu.roll(ext, width + 2 * LANES - 1, 1)[:, LANES : LANES + width]
            up = jnp.where(row == 0, S[above, H - 1 : H, cs], pltpu.roll(cur, 1, 0))
            down = jnp.where(row == H - 1, S[below, 0:1, cs], pltpu.roll(cur, H - 1, 0))
            field = (up + down) + (left + right)
            fresh = jnp.tanh(beta * field + N[sweep, i, :, cs].astype(jnp.float32))
            S[i, :, cs] = jnp.where(parity == colour, fresh, cur)

    def finish(t):
        i = t + 1

        R[me, t] = S[i, :, share_of(me)]
        total = jnp.zeros((H, LANES), jnp.float32)
        for b in range(cols // width):
            c0 = b * width
            cs = slice(c0, c0 + width)
            cur = S[i, :, cs]
            out_ref[0, pl.ds(pl.multiple_of(t * H, H), H), cs] = cur
            after = (c0 + width) % cols
            ext = jnp.concatenate([cur, S[i, :, after : after + LANES]], axis=1)
            right = pltpu.roll(ext, width + LANES - 1, 1)[:, :width]
            down = jnp.where(row == H - 1, S[i + 1, 0:1, cs], pltpu.roll(cur, H - 1, 0))
            total = total + fold_lanes(cur * (down + right))
        EP[t] = total

    def send(p):
        for d in range(1, n):
            bulk(p, d).start()

    loaded(0)
    loaded(1)

    @pl.loop(1, T + STAGES)
    def _(s):
        @pl.when((s + 1 < T) & (s < T // 2 - 1))
        def _():
            loaded(s + 1)

        @pl.when(s == T // 2 - 1)
        def _():
            @pl.loop(T // 2, T)
            def _(t):
                loaded(t)

        @pl.when(s == 2 * STAGES + GROUP - 1)
        def _():
            pl.semaphore_wait(barrier, n - 1 + peers - 1)

        @pl.when(s == T - 1)
        def _():
            for copy in halos[1 + SWEEPS :]:
                copy.wait_recv()
            for w in range(SWEEPS):
                N[w, T + 1] = NR[1, w].astype(jnp.bfloat16)

        for k in range(STAGES):
            t = s - k

            @pl.when((t >= k + 1) & (t <= T))
            def _():
                update(t, k)

        @pl.when(s - STAGES >= STAGES)
        def _():
            t = s - STAGES
            finish(t)

            @pl.when(lax.rem(t, GROUP) == GROUP - 1)
            def _():
                send(t // GROUP)

        @pl.when(s == T // 2)
        def _():
            for w in range(SWEEPS):
                NH[0, w] = N[w, T].astype(jnp.float32)
                NH[1, w] = N[w, 1].astype(jnp.float32)
            for copy in halos:
                copy.start()

    for copy in halos[: 1 + SWEEPS]:
        copy.wait_recv()
    for w in range(SWEEPS):
        N[w, 0] = NR[0, w].astype(jnp.bfloat16)

    for k in range(STAGES):

        @pl.loop(-1 if k < STAGES - 1 else 0, k + 1)
        def _(t):
            update(t, k)

    @pl.loop(0, STAGES)
    def _(t):
        finish(t)

    @pl.loop(0, STAGES // GROUP)
    def _(p):
        send(p)

    per_row = jnp.sum(EP[...].reshape(rows, LANES).T, axis=0, keepdims=True) * (-1.0 / cols)
    energy_ref[...] = per_row
    local = jnp.broadcast_to(jnp.sum(per_row, axis=1, keepdims=True), (8, LANES))
    EM[...] = local
    EG[tile] = local

    def energy_copy(d):
        return pltpu.make_async_remote_copy(
            EM, EG.at[tile], es_sem.at[d], er_sem.at[tile],
            device_id={"tile": lax.rem(tile + d, peers)}, device_id_type=MESH,
        )

    def energy_from(d):
        src = lax.rem(tile + d, peers)
        return pltpu.make_async_remote_copy(
            EM, EG.at[src], es_sem.at[d], er_sem.at[src], device_id={"tile": src}, device_id_type=MESH
        )

    @pl.loop(1, peers)
    def _(d):
        energy_copy(d).start()

    @pl.loop(1, peers)
    def _(d):
        energy_from(d).wait_recv()

    energy = jnp.sum(EG[...], axis=0) / total_rows
    line = lax.broadcasted_iota(jnp.int32, (8, LANES), 0)
    label_float = labels_ref[0].astype(jnp.float32)
    accept_zero = accept_ref[0, 0].astype(jnp.float32)
    accept_one = accept_ref[0, 1].astype(jnp.float32)
    message = jnp.where(
        line == 0, energy,
        jnp.where(line == 1, label_float, jnp.where(line == 2, accept_zero, accept_one)),
    )
    LM[...] = message
    LG[me] = message

    def ladder_copy(d):
        return pltpu.make_async_remote_copy(
            LM, LG.at[me], ls_sem.at[d], lr_sem.at[me],
            device_id={"rep": lax.rem(me + d, n)}, device_id_type=MESH,
        )

    def ladder_from(d):
        src = lax.rem(me + d, n)
        return pltpu.make_async_remote_copy(
            LM, LG.at[src], ls_sem.at[d], lr_sem.at[src], device_id={"rep": src}, device_id_type=MESH
        )

    @pl.loop(1, n)
    def _(d):
        ladder_copy(d).start()

    def bulk_from(d, p):
        src = lax.rem(me + d, n)
        return pltpu.make_async_remote_copy(
            S.at[pl.ds(1, GROUP), :, share_of(0)], R.at[src, pl.ds(p * GROUP, GROUP)],
            bs_sem.at[0, 1], br_sem.at[src, p], device_id={"rep": src}, device_id_type=MESH,
        )

    @pl.loop(STAGES // GROUP, (T + STAGES) // GROUP)
    def _(s):
        p = lax.rem(s, T // GROUP)
        for d in range(1, n):
            bulk_from(d, p).wait_recv()
        for g in range(GROUP):
            t = p * GROUP + g
            totals = [jnp.zeros((H, LANES), jnp.float32) for _ in range(n)]
            for b in range(share // LANES):
                cs = slice(b * LANES, (b + 1) * LANES)
                parts = [R[r, t, :, cs] for r in range(n)]
                for r in range(n):
                    totals[r] = totals[r] + parts[r] * parts[(r + 1) % n]
            for r in range(n):
                MP[r, t] = totals[r]

    for r in range(n):
        sums = jnp.sum(MP[r].reshape(rows, LANES).T, axis=0, keepdims=True)
        MS[r] = jnp.broadcast_to(sums, (8, rows))
    MR[me] = MS[me]

    def margin_copy(d):
        dest = lax.rem(me + d, n)
        return pltpu.make_async_remote_copy(
            MS.at[dest], MR.at[me], ms_sem.at[d], mr_sem.at[me], device_id={"rep": dest}, device_id_type=MESH
        )

    def margin_from(d):
        src = lax.rem(me + d, n)
        return pltpu.make_async_remote_copy(
            MS.at[0], MR.at[src], ms_sem.at[d], mr_sem.at[src], device_id={"rep": src}, device_id_type=MESH
        )

    for d in range(1, n):
        margin_copy(d).start()

    @pl.loop(1, n)
    def _(d):
        ladder_from(d).wait_recv()

    energies = [LG[r][0:1] for r in range(n)]
    labels = [LG[r][1:2] for r in range(n)]
    acc = [[LG[r][2 + p : 3 + p] for r in range(n)] for p in range(2)]

    def beta_of(label):
        value = jnp.zeros((1, LANES), jnp.float32)
        for k in range(n):
            value = value + jnp.where(label == float(k), betas_ref[k], 0.0)
        return value

    def swapped(current, accepts, first):
        result = list(current)
        for r in range(first, n, 2):
            o = (r + 1) % n
            take = accepts[r] == 1.0
            result[r] = jnp.where(take, current[o], current[r])
            result[o] = jnp.where(take, current[r], current[o])
        return result

    labels_one = swapped(labels, acc[0], 0)
    labels_two = swapped(labels_one, acc[1], 1)
    zero = [beta_of(x) for x in labels]
    one = [beta_of(x) for x in labels_one]
    two = [beta_of(x) for x in labels_two]
    my_label = jnp.zeros((1, LANES), jnp.float32)
    my_log = my_label
    my_beta = my_label
    for r in range(n):
        o = (r + 1) % n
        betas_here = zero if r % 2 == 0 else one
        log = (betas_here[r] - betas_here[o]) * (energies[r] - energies[o])
        my_label = jnp.where(me == r, labels_two[r], my_label)
        my_log = jnp.where(me == r, log, my_log)
        my_beta = jnp.where(me == r, two[r], my_beta)
    label_out[0] = jnp.max(my_label).astype(jnp.int32)
    log_out[0] = jnp.max(my_log)
    beta_out[0] = jnp.max(my_beta)

    for copy in halos:
        copy.wait_send()

    @pl.loop(0, T // GROUP)
    def _(p):
        for d in range(1, n):
            bulk(p, d).wait_send()

    @pl.loop(1, peers)
    def _(d):
        energy_copy(d).wait_send()

    for d in range(1, n):
        ladder_copy(d).wait_send()
        margin_from(d).wait_recv()
        margin_copy(d).wait_send()

    margin_ref[...] = jnp.sum(MR[...], axis=0)[0:1] * (1.0 / cols)


def settle(spins, *refs):
    count = (len(refs) - 2) // 2
    sources, out, outs = refs[:count], refs[count], refs[count + 1 : 2 * count + 1]
    sem = refs[2 * count + 1]
    copies = [
        pltpu.make_async_copy(a, b, sem.at[k]) for k, (a, b) in enumerate(zip((spins, *sources), (out, *outs)))
    ]
    for copy in copies:
        copy.start()
    for copy in copies:
        copy.wait()


def body(n, peers, total_rows, spins_in, noise, betas, labels, accept):
    _, rows, cols = spins_in.shape
    T = rows // H
    f32 = jnp.float32
    limit = VMEM_BYTES - 4 * rows * cols
    hbm = pl.BlockSpec(memory_space=pltpu.HBM)
    smem = pl.BlockSpec(memory_space=pltpu.SMEM)
    vmem = pl.BlockSpec(memory_space=pltpu.VMEM)
    dma = pltpu.SemaphoreType.DMA
    accept = jnp.transpose(accept)
    results = pl.pallas_call(
        functools.partial(kernel, n, peers, total_rows),
        out_shape=(
            pltpu.VMEM(spins_in.shape, f32),
            jax.ShapeDtypeStruct((1, rows), f32),
            jax.ShapeDtypeStruct((1, rows), f32),
            jax.ShapeDtypeStruct((1,), jnp.int32),
            jax.ShapeDtypeStruct((1,), f32),
            jax.ShapeDtypeStruct((1,), f32),
        ),
        in_specs=[hbm, hbm, hbm, smem, hbm],
        out_specs=(vmem, vmem, vmem, smem, smem, smem),
        scratch_shapes=[
            pltpu.VMEM((T + 2, H, cols), f32),
            pltpu.VMEM((SWEEPS, T + 2, H, cols), jnp.bfloat16),
            pltpu.VMEM((n, T, H, cols // n), f32),
            pltpu.VMEM((2, SWEEPS, H, cols), f32),
            pltpu.VMEM((2, SWEEPS, H, cols), f32),
            pltpu.VMEM((T, H, LANES), f32),
            pltpu.VMEM((n, T, H, LANES), f32),
            pltpu.VMEM((n, 8, rows), f32),
            pltpu.VMEM((n, 8, rows), f32),
            pltpu.VMEM((8, LANES), f32),
            pltpu.VMEM((peers, 8, LANES), f32),
            pltpu.VMEM((8, LANES), f32),
            pltpu.VMEM((n, 8, LANES), f32),
            pltpu.SMEM(betas.shape, f32),
            pltpu.SMEM(accept.shape, jnp.int32),
            dma((T,)),
            dma((SWEEPS, T)),
            dma((2, 1 + SWEEPS)),
            dma((2, 1 + SWEEPS)),
            dma((T // GROUP, n)),
            dma((n, T // GROUP)),
            dma((n,)),
            dma((n,)),
            dma((peers,)),
            dma((peers,)),
            dma((n,)),
            dma((n,)),
            dma((2,)),
        ],
        compiler_params=pltpu.CompilerParams(collective_id=0, has_side_effects=True, vmem_limit_bytes=limit),
        name="lattice_exchange",
    )(spins_in, noise, betas, labels, accept)
    return pl.pallas_call(
        settle,
        out_shape=tuple(jax.ShapeDtypeStruct(x.shape, x.dtype) for x in results),
        in_specs=[vmem] + [hbm] * (len(results) - 1),
        out_specs=(hbm,) * len(results),
        scratch_shapes=[dma((len(results),))],
        compiler_params=pltpu.CompilerParams(vmem_limit_bytes=VMEM_BYTES // 2),
        name="settle",
    )(*results)


def solution(mesh):
    n = mesh.shape["rep"]
    peers = mesh.shape["tile"]
    in_specs = (P("rep", "tile", None), P(None, "rep", "tile", None), P(), P("rep"), P(None, "rep"))
    out_specs = (P("rep", "tile", None), P("rep", "tile"), P("rep", "tile"), P("rep"), P("rep"), P("rep"))

    def run(spins_in, noise, betas, labels, accept):
        total_rows = spins_in.shape[1]
        step = jax.shard_map(
            functools.partial(body, n, peers, total_rows),
            mesh=mesh, in_specs=in_specs, out_specs=out_specs, check_vma=False,
        )
        return step(spins_in, noise, betas, labels, accept)

    return run
```

```python
import functools

import jax
import jax.numpy as jnp
from jax import lax
from jax.experimental import pallas as pl
from jax.experimental.pallas import tpu as pltpu
from jax.sharding import PartitionSpec as P

SWEEPS = 2
H = 8
GROUP = 2
LANES = 128
PIECES = 8
VMEM_BYTES = 60 * 1024 * 1024
STAGES = 2 * SWEEPS
MESH = pl.DeviceIdType.MESH


def fold_lanes(value):
    total = value[:, :LANES]
    for k in range(1, value.shape[1] // LANES):
        total = total + value[:, k * LANES : (k + 1) * LANES]
    return total


def with_sides(ref, t, start, width, cols):
    before = (start - LANES) % cols
    after = (start + width) % cols
    return jnp.concatenate(
        [
            ref[t, :, before : before + LANES],
            ref[t, :, start : start + width],
            ref[t, :, after : after + LANES],
        ],
        axis=1,
    )


def kernel(
    n, peers, total_rows,
    spins_ref, noise_ref, betas_hbm, labels_ref, accept_hbm,
    out_ref, energy_ref, margin_ref, small_ref,
    S, N, R, NH, NR, EP, MP, MS, MR, EM, EG, LM, LG, betas_ref, accept_ref,
    s_sem, n_sem, hs_sem, hr_sem, bs_sem, br_sem,
    ms_sem, mr_sem, es_sem, er_sem, ls_sem, lr_sem, i_sem,
):
    _, rows, cols = spins_ref.shape
    T = rows // H
    width = min(4096, cols)
    share = cols // n
    me = lax.axis_index("rep")
    tile = lax.axis_index("tile")
    nxt = lax.rem(tile + 1, peers)
    prv = lax.rem(tile + peers - 1, peers)

    def load_spins(t):
        return pltpu.make_async_copy(spins_ref.at[0, pl.ds(pl.multiple_of(t * H, H), H)], S.at[t + 1], s_sem.at[t])

    def load_noise(w, t):
        return pltpu.make_async_copy(
            noise_ref.at[w, 0, pl.ds(pl.multiple_of(t * H, H), H)], N.at[w, t + 1], n_sem.at[w, t]
        )

    def load(t):
        load_spins(t).start()
        for w in range(SWEEPS):
            load_noise(w, t).start()

    def loaded(t):
        load_spins(t).wait()
        for w in range(SWEEPS):
            load_noise(w, t).wait()

    barrier = pltpu.get_barrier_semaphore()

    @pl.loop(1, peers)
    def _(d):
        pl.semaphore_signal(barrier, inc=1, device_id={"tile": lax.rem(tile + d, peers)}, device_id_type=MESH)

    @pl.loop(1, n)
    def _(d):
        pl.semaphore_signal(barrier, inc=1, device_id={"rep": lax.rem(me + d, n)}, device_id_type=MESH)

    small = [
        pltpu.make_async_copy(src, dst, i_sem.at[k])
        for k, (src, dst) in enumerate(
            ((betas_hbm, betas_ref), (accept_hbm, accept_ref))
        )
    ]
    for copy in small:
        copy.start()
    @pl.loop(0, T)
    def _(t):
        load(t)

    for copy in small:
        copy.wait()
    beta = jnp.float32(0.0)
    for k in range(n):
        beta = beta + jnp.where(labels_ref[0] == k, betas_ref[k], 0.0)

    def halo_copies():
        copies = []
        for side, (start, slot, dev) in enumerate(((rows - H, 0, nxt), (0, T + 1, prv))):
            copies.append(
                pltpu.make_async_remote_copy(
                    spins_ref.at[0, pl.ds(start, H)], S.at[slot], hs_sem.at[side, 0], hr_sem.at[side, 0],
                    device_id={"tile": dev}, device_id_type=MESH,
                )
            )
            for w in range(SWEEPS):
                copies.append(
                    pltpu.make_async_remote_copy(
                        NH.at[side, w], NR.at[side, w], hs_sem.at[side, 1 + w], hr_sem.at[side, 1 + w],
                        device_id={"tile": dev}, device_id_type=MESH,
                    )
                )
        return copies

    halos = halo_copies()

    def share_of(d):
        return pl.ds(pl.multiple_of(d * share, LANES), share)

    def bulk(p, d):
        dest = lax.rem(me + d, n)
        return pltpu.make_async_remote_copy(
            S.at[pl.ds(p * GROUP + 1, GROUP), :, share_of(dest)], R.at[me, pl.ds(p * GROUP, GROUP)],
            bs_sem.at[p, d], br_sem.at[me, p],
            device_id={"rep": dest}, device_id_type=MESH,
        )

    row = lax.broadcasted_iota(jnp.int32, (H, width), 0)
    parity = (row + lax.broadcasted_iota(jnp.int32, (H, width), 1)) % 2

    def update(t, stage):
        sweep, colour = stage // 2, stage % 2
        i = t + 1
        above = jnp.maximum(i - 1, 0)
        below = jnp.minimum(i + 1, T + 1)
        for b in range(cols // width):
            c0 = b * width
            cs = slice(c0, c0 + width)
            cur = S[i, :, cs]
            left = pltpu.roll(cur, 1, 1)
            right = pltpu.roll(cur, cols - 1, 1)
            up = jnp.where(row == 0, S[above, H - 1 : H, cs], pltpu.roll(cur, 1, 0))
            down = jnp.where(row == H - 1, S[below, 0:1, cs], pltpu.roll(cur, H - 1, 0))
            field = (up + down) + (left + right)
            fresh = jnp.tanh(beta * field + N[sweep, i, :, cs].astype(jnp.float32))
            S[i, :, cs] = jnp.where(parity == colour, fresh, cur)

    def finish(t):
        i = t + 1

        R[me, t] = S[i, :, share_of(me)]
        total = jnp.zeros((H, LANES), jnp.float32)
        for b in range(cols // width):
            c0 = b * width
            cs = slice(c0, c0 + width)
            cur = S[i, :, cs]
            out_ref[0, pl.ds(pl.multiple_of(t * H, H), H), cs] = cur
            after = (c0 + width) % cols
            ext = jnp.concatenate([cur, S[i, :, after : after + LANES]], axis=1)
            right = pltpu.roll(ext, width + LANES - 1, 1)[:, :width]
            down = jnp.where(row == H - 1, S[i + 1, 0:1, cs], pltpu.roll(cur, H - 1, 0))
            total = total + fold_lanes(cur * (down + right))
        EP[t] = total

    def send(p):
        for d in range(1, n):
            bulk(p, d).start()

    loaded(0)
    loaded(1)

    @pl.loop(1, T + STAGES)
    def _(s):
        @pl.when((s + 1 < T) & (s < T // 2 - 1))
        def _():
            loaded(s + 1)

        @pl.when(s == T // 2 - 1)
        def _():
            @pl.loop(T // 2, T)
            def _(t):
                loaded(t)

        @pl.when(s == 2 * STAGES + GROUP - 1)
        def _():
            pl.semaphore_wait(barrier, n - 1 + peers - 1)

        @pl.when(s == T - 1)
        def _():
            for copy in halos[1 + SWEEPS :]:
                copy.wait_recv()
            for w in range(SWEEPS):
                N[w, T + 1] = NR[1, w].astype(jnp.bfloat16)

        for k in range(STAGES):
            t = s - k

            @pl.when((t >= k + 1) & (t <= T))
            def _():
                update(t, k)

        @pl.when(s - STAGES >= STAGES)
        def _():
            t = s - STAGES
            finish(t)

            @pl.when(lax.rem(t, GROUP) == GROUP - 1)
            def _():
                send(t // GROUP)

        @pl.when(s == T // 2)
        def _():
            for w in range(SWEEPS):
                NH[0, w] = N[w, T].astype(jnp.float32)
                NH[1, w] = N[w, 1].astype(jnp.float32)
            for copy in halos:
                copy.start()

    for copy in halos[: 1 + SWEEPS]:
        copy.wait_recv()
    for w in range(SWEEPS):
        N[w, 0] = NR[0, w].astype(jnp.bfloat16)

    for k in range(STAGES):

        @pl.loop(-1 if k < STAGES - 1 else 0, k + 1)
        def _(t):
            update(t, k)

    @pl.loop(0, STAGES)
    def _(t):
        finish(t)


    per_row = jnp.sum(EP[...].reshape(rows, LANES).T, axis=0, keepdims=True) * (-1.0 / cols)
    energy_ref[...] = per_row
    local = jnp.broadcast_to(jnp.sum(per_row, axis=1, keepdims=True), (8, LANES))
    EM[...] = local
    EG[tile] = local

    def energy_copy(d):
        return pltpu.make_async_remote_copy(
            EM, EG.at[tile], es_sem.at[d], er_sem.at[tile],
            device_id={"tile": lax.rem(tile + d, peers)}, device_id_type=MESH,
        )

    def energy_from(d):
        src = lax.rem(tile + d, peers)
        return pltpu.make_async_remote_copy(
            EM, EG.at[src], es_sem.at[d], er_sem.at[src], device_id={"tile": src}, device_id_type=MESH
        )

    @pl.loop(1, peers)
    def _(d):
        energy_copy(d).start()

    @pl.loop(1, peers)
    def _(d):
        energy_from(d).wait_recv()

    energy = jnp.sum(EG[...], axis=0) / total_rows
    line = lax.broadcasted_iota(jnp.int32, (8, LANES), 0)
    label_float = labels_ref[0].astype(jnp.float32)
    accept_zero = accept_ref[0, 0].astype(jnp.float32)
    accept_one = accept_ref[0, 1].astype(jnp.float32)
    message = jnp.where(
        line == 0, energy,
        jnp.where(line == 1, label_float, jnp.where(line == 2, accept_zero, accept_one)),
    )
    LM[...] = message
    LG[me] = message

    def ladder_copy(d):
        return pltpu.make_async_remote_copy(
            LM, LG.at[me], ls_sem.at[d], lr_sem.at[me],
            device_id={"rep": lax.rem(me + d, n)}, device_id_type=MESH,
        )

    def ladder_from(d):
        src = lax.rem(me + d, n)
        return pltpu.make_async_remote_copy(
            LM, LG.at[src], ls_sem.at[d], lr_sem.at[src], device_id={"rep": src}, device_id_type=MESH
        )

    @pl.loop(1, n)
    def _(d):
        ladder_copy(d).start()

    @pl.loop(0, STAGES // GROUP)
    def _(p):
        send(p)

    def bulk_from(d, p):
        src = lax.rem(me + d, n)
        return pltpu.make_async_remote_copy(
            S.at[pl.ds(1, GROUP), :, share_of(0)], R.at[src, pl.ds(p * GROUP, GROUP)],
            bs_sem.at[0, 1], br_sem.at[src, p], device_id={"rep": src}, device_id_type=MESH,
        )

    def margins(p):
        for d in range(1, n):
            bulk_from(d, p).wait_recv()
        for g in range(GROUP):
            t = p * GROUP + g
            totals = [jnp.zeros((H, LANES), jnp.float32) for _ in range(n)]
            for b in range(share // LANES):
                cs = slice(b * LANES, (b + 1) * LANES)
                parts = [R[r, t, :, cs] for r in range(n)]
                for r in range(n):
                    totals[r] = totals[r] + parts[r] * parts[(r + 1) % n]
            for r in range(n):
                MP[r, t] = totals[r]

    def margin_sums(first, last):
        for r in range(n):
            part = MP[r, first:last].reshape((last - first) * H, LANES)
            sums = jnp.sum(part.T, axis=0, keepdims=True)
            MS[r, :, first * H : last * H] = jnp.broadcast_to(sums, (8, (last - first) * H))

    @pl.loop(STAGES // GROUP, T // GROUP)
    def _(p):
        margins(p)

    split = LANES // H
    if split < T:
        margin_sums(split, T)

    @pl.loop(1, n)
    def _(d):
        ladder_from(d).wait_recv()

    energies = [LG[r][0:1] for r in range(n)]
    labels = [LG[r][1:2] for r in range(n)]
    acc = [[LG[r][2 + p : 3 + p] for r in range(n)] for p in range(2)]

    def beta_of(label):
        value = jnp.zeros((1, LANES), jnp.float32)
        for k in range(n):
            value = value + jnp.where(label == float(k), betas_ref[k], 0.0)
        return value

    def swapped(current, accepts, first):
        result = list(current)
        for r in range(first, n, 2):
            o = (r + 1) % n
            take = accepts[r] == 1.0
            result[r] = jnp.where(take, current[o], current[r])
            result[o] = jnp.where(take, current[r], current[o])
        return result

    labels_one = swapped(labels, acc[0], 0)
    labels_two = swapped(labels_one, acc[1], 1)
    zero = [beta_of(x) for x in labels]
    one = [beta_of(x) for x in labels_one]
    two = [beta_of(x) for x in labels_two]
    my_label = jnp.zeros((1, LANES), jnp.float32)
    my_log = my_label
    my_beta = my_label
    for r in range(n):
        o = (r + 1) % n
        betas_here = zero if r % 2 == 0 else one
        log = (betas_here[r] - betas_here[o]) * (energies[r] - energies[o])
        my_label = jnp.where(me == r, labels_two[r], my_label)
        my_log = jnp.where(me == r, log, my_log)
        my_beta = jnp.where(me == r, two[r], my_beta)
    small_ref[...] = jnp.concatenate([my_label, my_log, my_beta, jnp.zeros((5, LANES), jnp.float32)], axis=0)

    @pl.loop(0, STAGES // GROUP)
    def _(p):
        margins(p)

    margin_sums(0, min(split, T))
    MR[me] = MS[me]

    def margin_copy(d):
        dest = lax.rem(me + d, n)
        return pltpu.make_async_remote_copy(
            MS.at[dest], MR.at[me], ms_sem.at[d], mr_sem.at[me], device_id={"rep": dest}, device_id_type=MESH
        )

    def margin_from(d):
        src = lax.rem(me + d, n)
        return pltpu.make_async_remote_copy(
            MS.at[0], MR.at[src], ms_sem.at[d], mr_sem.at[src], device_id={"rep": src}, device_id_type=MESH
        )

    for d in range(1, n):
        margin_copy(d).start()

    for copy in halos:
        copy.wait_send()

    @pl.loop(0, T // GROUP)
    def _(p):
        for d in range(1, n):
            bulk(p, d).wait_send()

    @pl.loop(1, peers)
    def _(d):
        energy_copy(d).wait_send()

    for d in range(1, n):
        ladder_copy(d).wait_send()
        margin_from(d).wait_recv()
        margin_copy(d).wait_send()

    margin_ref[...] = jnp.sum(MR[...], axis=0)[0:1] * (1.0 / cols)


def settle(spins, energy, margin, small, *refs):
    spins_out, energy_out, margin_out, label_out, log_out, beta_out = refs[:6]
    label, log, beta, sem = refs[6:]
    height = spins.shape[1] // PIECES
    pairs = [(energy, energy_out), (margin, margin_out)]
    pairs += [
        (spins.at[0, pl.ds(k * height, height)], spins_out.at[0, pl.ds(k * height, height)]) for k in range(PIECES)
    ]
    pairs += [(label, label_out), (log, log_out), (beta, beta_out)]
    copies = [pltpu.make_async_copy(a, b, sem.at[k]) for k, (a, b) in enumerate(pairs)]
    for copy in copies[:-3]:
        copy.start()
    label[0] = jnp.max(small[0:1]).astype(jnp.int32)
    log[0] = jnp.max(small[1:2])
    beta[0] = jnp.max(small[2:3])
    for copy in copies[-3:]:
        copy.start()
    for copy in copies:
        copy.wait()


def body(n, peers, total_rows, spins_in, noise, betas, labels, accept):
    _, rows, cols = spins_in.shape
    T = rows // H
    f32 = jnp.float32
    limit = VMEM_BYTES - 4 * (rows * cols + 2 * rows + 8 * LANES)
    hbm = pl.BlockSpec(memory_space=pltpu.HBM)
    smem = pl.BlockSpec(memory_space=pltpu.SMEM)
    vmem = pl.BlockSpec(memory_space=pltpu.VMEM)
    dma = pltpu.SemaphoreType.DMA
    accept = jnp.transpose(accept)
    results = pl.pallas_call(
        functools.partial(kernel, n, peers, total_rows),
        out_shape=(
            pltpu.VMEM(spins_in.shape, f32),
            pltpu.VMEM((1, rows), f32),
            pltpu.VMEM((1, rows), f32),
            pltpu.VMEM((8, LANES), f32),
        ),
        in_specs=[hbm, hbm, hbm, smem, hbm],
        out_specs=(vmem,) * 4,
        scratch_shapes=[
            pltpu.VMEM((T + 2, H, cols), f32),
            pltpu.VMEM((SWEEPS, T + 2, H, cols), jnp.bfloat16),
            pltpu.VMEM((n, T, H, cols // n), f32),
            pltpu.VMEM((2, SWEEPS, H, cols), f32),
            pltpu.VMEM((2, SWEEPS, H, cols), f32),
            pltpu.VMEM((T, H, LANES), f32),
            pltpu.VMEM((n, T, H, LANES), f32),
            pltpu.VMEM((n, 8, rows), f32),
            pltpu.VMEM((n, 8, rows), f32),
            pltpu.VMEM((8, LANES), f32),
            pltpu.VMEM((peers, 8, LANES), f32),
            pltpu.VMEM((8, LANES), f32),
            pltpu.VMEM((n, 8, LANES), f32),
            pltpu.SMEM(betas.shape, f32),
            pltpu.SMEM(accept.shape, jnp.int32),
            dma((T,)),
            dma((SWEEPS, T)),
            dma((2, 1 + SWEEPS)),
            dma((2, 1 + SWEEPS)),
            dma((T // GROUP, n)),
            dma((n, T // GROUP)),
            dma((n,)),
            dma((n,)),
            dma((peers,)),
            dma((peers,)),
            dma((n,)),
            dma((n,)),
            dma((2,)),
        ],
        compiler_params=pltpu.CompilerParams(collective_id=0, has_side_effects=True, vmem_limit_bytes=limit),
        name="lattice_exchange",
    )(spins_in, noise, betas, labels, accept)
    return pl.pallas_call(
        settle,
        out_shape=(
            jax.ShapeDtypeStruct(spins_in.shape, f32),
            jax.ShapeDtypeStruct((1, rows), f32),
            jax.ShapeDtypeStruct((1, rows), f32),
            jax.ShapeDtypeStruct((1,), jnp.int32),
            jax.ShapeDtypeStruct((1,), f32),
            jax.ShapeDtypeStruct((1,), f32),
        ),
        in_specs=[vmem] * 4,
        out_specs=(hbm,) * 6,
        scratch_shapes=[
            pltpu.SMEM((1,), jnp.int32),
            pltpu.SMEM((1,), f32),
            pltpu.SMEM((1,), f32),
            dma((PIECES + 5,)),
        ],
        compiler_params=pltpu.CompilerParams(vmem_limit_bytes=VMEM_BYTES // 2),
        name="settle",
    )(*results)


def solution(mesh):
    n = mesh.shape["rep"]
    peers = mesh.shape["tile"]
    in_specs = (P("rep", "tile", None), P(None, "rep", "tile", None), P(), P("rep"), P(None, "rep"))
    out_specs = (P("rep", "tile", None), P("rep", "tile"), P("rep", "tile"), P("rep"), P("rep"), P("rep"))

    def run(spins_in, noise, betas, labels, accept):
        total_rows = spins_in.shape[1]
        step = jax.shard_map(
            functools.partial(body, n, peers, total_rows),
            mesh=mesh, in_specs=in_specs, out_specs=out_specs, check_vma=False,
        )
        return step(spins_in, noise, betas, labels, accept)

    return run
```
